32 devices in a mesh: member: 8 (over z, y), band: 4 (over x, core).
Axes of the slice: x: 2, y: 2, z: 4, core: 2. Of those that a mesh axis runs over, the one named last changes fastest.
Arguments:
- spectral: float32 [128, 768, 768], P('member', 'band'), parts along dimension 0, may hold values from -6 to 6
- coupling: float32 [8192, 1024], P(('member', 'band')), parts along dimension 0, may hold values from 0.02 to 162, as said below
- quadratic: float32 [8192, 1024], P(('member', 'band')), parts along dimension 0, may hold values from -1.5 to 1.5
Outputs:
- tendency_spectral: float32 [128, 768, 768], P('member', 'band'), parts along dimension 0
The draws below stay inside these ranges and needn't reach their ends.
There are 8 independent parts, one for each index of `member`. The reference program is written for one: setup_inputs(seed, part) draws one part's arguments, and reference() takes and returns one part's arrays. A program takes and returns all parts, laid end to end along the dimension named above; each array names one. Nothing has to cross between parts.
Inputs may be any that keep to these rules, and one draw needn't show every extreme that they name: `coupling`: positive.
All inputs are finite; a program needn't handle non-finite values.
Results may differ from the reference program's by a relative error of at most 0.00008.
Values sent between devices are 32-bit elements; how exact they have to be, the bound alone decides.
A program may use at most 128 MiB of HBM per device.

```python
import math
import jax
import jax.numpy as jnp
from jax import lax

N = 1024
LEVELS = 16
KS = 768


def draw_coupling(key, part):
    keys = jax.random.split(jax.random.fold_in(key, 11), 3)
    rows = jnp.arange(N, dtype=jnp.float32) / N
    row_noise = jax.random.uniform(keys[0], (N,), jnp.float32)
    col_noise = jax.random.uniform(keys[1], (N,), jnp.float32)
    trend = jnp.exp(jnp.log(3.0) * rows)
    cell = jax.random.uniform(keys[2], (N, N), jnp.float32, 0.5, 1.5)
    row_scale = trend * jnp.exp(jnp.log(10.0) * row_noise)
    col_scale = jnp.exp(jnp.log(10.0) * col_noise)
    return (row_scale[:, None] * col_scale[None, :] * cell / 10.0).astype(jnp.float32)


def block_levels(stream_key, extent, shards, smallest, largest):
    def one(dim, shards_of):
        steps = jax.random.uniform(jax.random.fold_in(jax.random.fold_in(stream_key, 6), dim), (shards_of,), jnp.float32, smallest / len(shards), largest / len(shards))
        return jnp.repeat(jnp.exp(steps), extent[dim] // shards_of).reshape((-1,) + (1,) * (len(extent) - dim - 1))

    gain = one(*shards[0])
    for cut in shards[1:]:
        gain = gain * one(*cut)
    return gain


def noise(stream_key, shape, deviation, most, cuts=(), kind=jnp.bfloat16):
    result = deviation * jax.random.normal(stream_key, shape, jnp.float32)
    if cuts:
        result = result * block_levels(stream_key, shape, cuts, -0.22, 0.18)
    return jnp.clip(result, -most, most).astype(kind)


def setup_inputs(seed: int = 0, part: int = 0) -> dict:
    seeds = jax.random.split(jax.random.key(seed), 4)
    part_splits = jax.random.split(jax.random.fold_in(seeds[3], part), 4)
    spectral = noise(part_splits[0], (LEVELS, KS, KS), 1.0, 6.0, ((1, 4),), jnp.float32)
    coupling = draw_coupling(jax.random.fold_in(jax.random.fold_in(seeds[3], part), 71), part)
    quadratic = noise(part_splits[2], (N, N), 0.25, 1.5, ((0, 4),), jnp.float32)
    return {"spectral": spectral, "coupling": coupling, "quadratic": quadratic}


def tables(cells, coeffs):
    half_count = coeffs // 2
    position = jnp.arange(cells, dtype=jnp.int32)
    column = jnp.arange(coeffs, dtype=jnp.int32)
    wavenumber = jnp.where(column < half_count, column, column - half_count)
    turns = position[:, None] * wavenumber[None, :] % cells
    angles = turns.astype(jnp.float32) * (2.0 * math.pi / cells)
    basis_table = jnp.where(column[None, :] < half_count, jnp.cos(angles), jnp.sin(angles))
    synthesis = basis_table / math.sqrt(half_count)
    factor = jnp.where(wavenumber == 0, 1.0, 2.0) * (math.sqrt(half_count) / cells)
    analysis = (basis_table * factor[None, :]).T
    return (synthesis, analysis)

def reference(spectral, coupling, quadratic):
    synthesis, analysis = tables(N, KS)
    high = lax.Precision.HIGHEST
    section = jnp.einsum('lab,yb->lay', spectral, synthesis, precision=high)
    grid = jnp.einsum('xa,lay->lyx', synthesis, section, precision=high)
    product = coupling[None] * grid
    energy = lax.optimization_barrier(jnp.mean(product * product, axis=(1, 2)))
    scaled = product / jnp.sqrt(energy + 1e-06)[:, None, None]
    tendency = scaled + quadratic[None] * scaled * scaled
    back = jnp.einsum('ax,lyx->lya', analysis, tendency, precision=high)
    return jnp.einsum('by,lya->lab', analysis, back, precision=high)
```

```python
import functools
import math

import jax
import jax.numpy as jnp
import numpy as np
from jax import lax
from jax.experimental import pallas as pl
from jax.experimental.pallas import tpu as pltpu
from jax.sharding import PartitionSpec as P

MESH = pl.DeviceIdType.MESH
F32 = jnp.float32
BF16 = jnp.bfloat16
LANES = 128
ROWS = 32
TILE = 256


def seeds(cells, coeffs):
    half = coeffs // 2
    wave = np.arange(half)

    def pair(points, transposed):
        turns = np.outer(points, wave) % cells
        angles = turns * (2.0 * math.pi / cells)
        both = np.stack([np.cos(angles), np.sin(angles)])
        return np.swapaxes(both, 1, 2).astype(np.float32) if transposed else both.astype(np.float32)

    return (
        pair(np.arange(0, cells, ROWS), False),
        pair(np.arange(ROWS), False),
        pair(np.arange(0, cells, LANES), True),
        pair(np.arange(LANES), True),
    )


def split(value):
    high = value.astype(BF16)
    return high, (value - high.astype(F32)).astype(BF16)


def dot3(a_high, a_low, b_high, b_low):
    dot = functools.partial(jnp.dot, preferred_element_type=F32)
    return dot(a_high, b_high) + dot(a_low, b_high) + dot(a_high, b_low)


def round_trip(
    ways, spectral, coupling, quadratic, coarse_r, fine_r, coarse_l, fine_l, out,
    fields, natural, turned, basis_h, basis_l, basis_th, basis_tl,
    field_h, field_l, half_h, half_l, product, tend_h, tend_l, back_h, back_l, total, result,
    fs, fr, fo, cs, cr, co, rs, bs, br, bo,
):
    levels, band, coeffs = spectral.shape
    rows, cells = coupling.shape
    half = coeffs // 2
    groups = levels // ways
    cores = 2 if ways % 2 == 0 else 1
    chips = ways // cores
    me = lax.axis_index("band")
    chip, core = me // cores, me % cores

    def partner(away, side):
        return ((chip + away) % chips) * cores + (core + side) % cores

    def band_of(index):
        return pl.ds(pl.multiple_of(index * band, band), band)

    def rows_of(index):
        return pl.ds(pl.multiple_of(index * rows, rows), rows)

    def send_field(group, to):
        return pltpu.make_async_remote_copy(
            src_ref=spectral.at[group * ways + to],
            dst_ref=fields.at[group, band_of(me)],
            send_sem=fs.at[group, to],
            recv_sem=fr.at[group, me],
            device_id={"band": to},
            device_id_type=MESH,
        )

    def take_field(group, source):
        return pltpu.make_async_remote_copy(
            src_ref=spectral.at[group * ways + me],
            dst_ref=fields.at[group, band_of(source)],
            send_sem=fs.at[group, source],
            recv_sem=fr.at[group, source],
            device_id={"band": source},
            device_id_type=MESH,
        )

    def own_field(group):
        return pltpu.make_async_copy(
            spectral.at[group * ways + me], fields.at[group, band_of(me)], fo.at[group]
        )

    weights = (coupling, quadratic)

    def send_weight(which, to):
        return pltpu.make_async_remote_copy(
            src_ref=weights[which],
            dst_ref=natural.at[which, rows_of(me)],
            send_sem=cs.at[which, to],
            recv_sem=cr.at[which, me],
            device_id={"band": to},
            device_id_type=MESH,
        )

    def take_weight(which, source):
        return pltpu.make_async_remote_copy(
            src_ref=weights[which],
            dst_ref=natural.at[which, rows_of(source)],
            send_sem=cs.at[which, source],
            recv_sem=cr.at[which, source],
            device_id={"band": source},
            device_id_type=MESH,
        )

    def relay_weight(which, source, to):
        return pltpu.make_async_remote_copy(
            src_ref=natural.at[which, rows_of(source)],
            dst_ref=natural.at[which, rows_of(source)],
            send_sem=rs.at[which, source],
            recv_sem=cr.at[which, source],
            device_id={"band": to},
            device_id_type=MESH,
        )

    def own_weight(which):
        return pltpu.make_async_copy(weights[which], natural.at[which, rows_of(me)], co.at[which])

    def send_result(group, to):
        return pltpu.make_async_remote_copy(
            src_ref=result.at[group, band_of(to)],
            dst_ref=out.at[group * ways + me],
            send_sem=bs.at[group, to],
            recv_sem=br.at[group, me],
            device_id={"band": to},
            device_id_type=MESH,
        )

    def take_result(group, source):
        return pltpu.make_async_remote_copy(
            src_ref=result.at[group, band_of(source)],
            dst_ref=out.at[group * ways + source],
            send_sem=bs.at[group, source],
            recv_sem=br.at[group, source],
            device_id={"band": source},
            device_id_type=MESH,
        )

    def own_result(group):
        return pltpu.make_async_copy(
            result.at[group, band_of(me)], out.at[group * ways + me], bo.at[group]
        )

    def step_partner(step):
        return partner((step // cores + 1) % chips, cores - 1 - step % cores)

    barrier = pltpu.get_barrier_semaphore()
    for step in range(ways - 1):
        pl.semaphore_signal(barrier, inc=1, device_id={"band": step_partner(step)}, device_id_type=MESH)
    pl.semaphore_wait(barrier, ways - 1)

    def start_fields(group):
        for step in range(ways - 1):
            send_field(group, step_partner(step)).start()
        own_field(group).start()

    start_fields(0)
    for which in range(2):
        for away in range(1, chips):
            send_weight(which, partner(away, 0)).start()
        for side in range(1, cores):
            send_weight(which, partner(0, side)).start()
        own_weight(which).start()
    for group in range(1, groups):
        start_fields(group)

    def rows_table(block, _):
        one, at = pl.ds(block, 1), pl.ds(pl.multiple_of(block * ROWS, ROWS), ROWS)
        cos_u, sin_u = coarse_r[0, one, :], coarse_r[1, one, :]
        cos_v, sin_v = fine_r[0], fine_r[1]
        high, low = split(cos_u * cos_v - sin_u * sin_v)
        basis_h[at, :half], basis_l[at, :half] = high, low
        high, low = split(sin_u * cos_v + cos_u * sin_v)
        basis_h[at, half:], basis_l[at, half:] = high, low
        return _

    lax.fori_loop(0, cells // ROWS, rows_table, 0)
    chunk = half // 6 if half % 96 == 0 else half

    def lanes_table(block, _):
        at = pl.ds(pl.multiple_of(block * chunk, chunk), chunk)
        below = pl.ds(pl.multiple_of(half + block * chunk, chunk), chunk)
        cos_v, sin_v = fine_l[0, at, :], fine_l[1, at, :]
        cos_w, sin_w = coarse_l[0, at, :], coarse_l[1, at, :]
        for word in range(cells // LANES):
            lanes = slice(word * LANES, (word + 1) * LANES)
            cos_u, sin_u = cos_w[:, word : word + 1], sin_w[:, word : word + 1]
            high, low = split(cos_u * cos_v - sin_u * sin_v)
            basis_th[at, lanes], basis_tl[at, lanes] = high, low
            high, low = split(sin_u * cos_v + cos_u * sin_v)
            basis_th[below, lanes], basis_tl[below, lanes] = high, low
        return _

    lax.fori_loop(0, half // chunk, lanes_table, 0)

    def factor(index):
        wave = jnp.where(index < half, index, index - half)
        return jnp.where(wave == 0, 1.0, 2.0) / cells

    def tile(index):
        return pl.ds(pl.multiple_of(index * TILE, TILE), TILE)

    def one_level(group, first):
        for step in range(ways - 1):
            take_field(group, step_partner(step)).wait_recv()
        own_field(group).wait()

        def split_field(index, _):
            at = band_of(index)
            field_h[at, :], field_l[at, :] = split(fields[group, at, :])
            return _

        lax.fori_loop(0, ways, split_field, 0)

        def synth_x(index, _):
            at = tile(index)
            value = dot3(basis_h[at, :], basis_l[at, :], field_h[...], field_l[...])
            half_h[at, :], half_l[at, :] = split(value)
            return _

        lax.fori_loop(0, cells // TILE, synth_x, 0)

        if first:
            for which in range(2):
                for away in range(1, chips):
                    take_weight(which, partner(away, 0)).wait_recv()
                    for side in range(1, cores):
                        relay_weight(which, partner(away, 0), partner(0, side)).start()
                for side in range(1, cores):
                    take_weight(which, partner(0, side)).wait_recv()
                own_weight(which).wait()
            for which in range(2):
                for away in range(1, chips):
                    for side in range(1, cores):
                        take_weight(which, partner(away, side)).wait_recv()

                def turn(index, _):
                    at = pl.ds(pl.multiple_of(index * LANES, LANES), LANES)
                    value = natural[which, at, :].T
                    turned[which, :, at] = value * (1.0 / half) if which == 0 else value
                    return _

                lax.fori_loop(0, cells // LANES, turn, 0)

        total[...] = jnp.zeros_like(total)

        def synth_y(index, _):
            at = tile(index)
            value = dot3(half_h[at, :], half_l[at, :], basis_th[...], basis_tl[...])
            value = value * turned[0, at, :]
            product[at, :] = value
            total[...] += jnp.sum((value * value).reshape(TILE // 8, 8, cells), axis=0)
            return _

        lax.fori_loop(0, cells // TILE, synth_y, 0)
        energy = jnp.sum(jnp.sum(total[...], axis=0, keepdims=True), axis=1, keepdims=True)
        scale = 1.0 / jnp.sqrt(energy * (1.0 / (cells * cells)) + 1e-06)

        def nonlinear(index, _):
            at = tile(index)
            scaled = product[at, :] * scale
            tend_h[at, :], tend_l[at, :] = split(scaled + turned[1, at, :] * scaled * scaled)
            return _

        lax.fori_loop(0, cells // TILE, nonlinear, 0)

        def analyse_x(index, _):
            at = tile(index)
            value = dot3(basis_th[at, :], basis_tl[at, :], tend_h[...], tend_l[...])
            back_h[at, :], back_l[at, :] = split(value)
            return _

        lax.fori_loop(0, coeffs // TILE, analyse_x, 0)
        columns = factor(lax.broadcasted_iota(jnp.int32, (1, coeffs), 1)) * half

        def analyse_y(step, _):
            to = step_partner(step)
            at = band_of(to)
            value = dot3(back_h[at, :], back_l[at, :], basis_h[...], basis_l[...])
            line = factor(lax.broadcasted_iota(jnp.int32, (band, 1), 0) + to * band)
            result[group, at, :] = value * (line * columns)

            @pl.when(step > 0)
            def _send():
                send_result(group, step_partner(step - 1)).start()

            return _

        lax.fori_loop(0, ways, analyse_y, 0)
        own_result(group).start()

    one_level(0, True)
    if groups > 1:

        def later(group, _):
            one_level(group, False)
            return _

        lax.fori_loop(1, groups, later, 0)

    def finish(group, _):
        for step in range(ways - 1):
            other = step_partner(step)
            send_field(group, other).wait_send()
            send_result(group, other).wait_send()
            take_result(group, other).wait_recv()
        own_result(group).wait()
        return _

    for which in range(2):
        for away in range(1, chips):
            send_weight(which, partner(away, 0)).wait_send()
            for side in range(1, cores):
                relay_weight(which, partner(away, 0), partner(0, side)).wait_send()
        for side in range(1, cores):
            send_weight(which, partner(0, side)).wait_send()
    lax.fori_loop(0, groups, finish, 0)


def on_device(spectral, coupling, quadratic):
    levels, band, coeffs = spectral.shape
    rows, cells = coupling.shape
    ways = lax.axis_size("band")
    groups = levels // ways
    anywhere = pl.BlockSpec(memory_space=pl.ANY)
    inside = pl.BlockSpec(memory_space=pltpu.VMEM)
    copies = pltpu.SemaphoreType.DMA
    return pl.pallas_call(
        functools.partial(round_trip, ways),
        out_shape=jax.ShapeDtypeStruct((levels, band, coeffs), F32),
        in_specs=[anywhere] * 3 + [inside] * 4,
        out_specs=anywhere,
        scratch_shapes=[
            pltpu.VMEM((groups, coeffs, coeffs), F32),
            pltpu.VMEM((2, cells, cells), F32),
            pltpu.VMEM((2, cells, cells), F32),
            pltpu.VMEM((cells, coeffs), BF16),
            pltpu.VMEM((cells, coeffs), BF16),
            pltpu.VMEM((coeffs, cells), BF16),
            pltpu.VMEM((coeffs, cells), BF16),
            pltpu.VMEM((coeffs, coeffs), BF16),
            pltpu.VMEM((coeffs, coeffs), BF16),
            pltpu.VMEM((cells, coeffs), BF16),
            pltpu.VMEM((cells, coeffs), BF16),
            pltpu.VMEM((cells, cells), F32),
            pltpu.VMEM((cells, cells), BF16),
            pltpu.VMEM((cells, cells), BF16),
            pltpu.VMEM((coeffs, cells), BF16),
            pltpu.VMEM((coeffs, cells), BF16),
            pltpu.VMEM((8, cells), F32),
            pltpu.VMEM((groups, coeffs, coeffs), F32),
            copies((groups, ways)),
            copies((groups, ways)),
            copies((groups,)),
            copies((2, ways)),
            copies((2, ways)),
            copies((2,)),
            copies((2, ways)),
            copies((groups, ways)),
            copies((groups, ways)),
            copies((groups,)),
        ],
        compiler_params=pltpu.CompilerParams(
            collective_id=0, has_side_effects=True, vmem_limit_bytes=67043328
        ),
        name="round_trip",
    )(spectral, coupling, quadratic, *seeds(cells, coeffs))


def solution(mesh):
    placed = (P("member", "band", None), P(("member", "band"), None), P(("member", "band"), None))
    return jax.shard_map(
        on_device, mesh=mesh, in_specs=placed, out_specs=P("member", "band", None), check_vma=False
    )
```

```python
import functools
import math

import jax
import jax.numpy as jnp
import numpy as np
from jax import lax
from jax.experimental import pallas as pl
from jax.experimental.pallas import tpu as pltpu
from jax.sharding import PartitionSpec as P

MESH = pl.DeviceIdType.MESH
F32 = jnp.float32
BF16 = jnp.bfloat16
LANES = 128
ROWS = 32
TILE = 256


def seeds(cells, coeffs):
    half = coeffs // 2
    wave = np.arange(half)

    def pair(points, transposed):
        turns = np.outer(points, wave) % cells
        angles = turns * (2.0 * math.pi / cells)
        both = np.stack([np.cos(angles), np.sin(angles)])
        return np.swapaxes(both, 1, 2).astype(np.float32) if transposed else both.astype(np.float32)

    return (
        pair(np.arange(0, cells, ROWS), False),
        pair(np.arange(ROWS), False),
        pair(np.arange(0, cells, LANES), True),
        pair(np.arange(LANES), True),
    )


def split(value):
    high = value.astype(BF16)
    return high, (value - high.astype(F32)).astype(BF16)


def dot3(a_high, a_low, b_high, b_low):
    dot = functools.partial(jnp.dot, preferred_element_type=F32)
    return dot(a_high, b_high) + dot(a_low, b_high) + dot(a_high, b_low)


def round_trip(
    ways, spectral, coupling, quadratic, seed_cr, seed_fr, seed_cl, seed_fl, out,
    coarse_r, fine_r, coarse_l, fine_l, fields, natural, turned, basis_h, basis_l, basis_th, basis_tl,
    field_h, field_l, half_h, half_l, tend_h, tend_l, back_h, back_l, total,
    ss, fs, fr, fo, cs, cr, co, rs, bs, br, bo,
):
    levels, band, coeffs = spectral.shape
    rows, cells = coupling.shape
    half = coeffs // 2
    groups = levels // ways
    cores = 2 if ways % 2 == 0 else 1
    chips = ways // cores
    me = lax.axis_index("band")
    chip, core = me // cores, me % cores

    def partner(away, side):
        return ((chip + away) % chips) * cores + (core + side) % cores

    def band_of(index):
        return pl.ds(pl.multiple_of(index * band, band), band)

    def rows_of(index):
        return pl.ds(pl.multiple_of(index * rows, rows), rows)

    def send_field(group, to):
        return pltpu.make_async_remote_copy(
            src_ref=spectral.at[group * ways + to],
            dst_ref=fields.at[group, band_of(me)],
            send_sem=fs.at[group, to],
            recv_sem=fr.at[group, me],
            device_id={"band": to},
            device_id_type=MESH,
        )

    def take_field(group, source):
        return pltpu.make_async_remote_copy(
            src_ref=spectral.at[group * ways + me],
            dst_ref=fields.at[group, band_of(source)],
            send_sem=fs.at[group, source],
            recv_sem=fr.at[group, source],
            device_id={"band": source},
            device_id_type=MESH,
        )

    def own_field(group):
        return pltpu.make_async_copy(
            spectral.at[group * ways + me], fields.at[group, band_of(me)], fo.at[group]
        )

    weights = (coupling, quadratic)

    def send_weight(which, to):
        return pltpu.make_async_remote_copy(
            src_ref=weights[which],
            dst_ref=natural.at[which, rows_of(me)],
            send_sem=cs.at[which, to],
            recv_sem=cr.at[which, me],
            device_id={"band": to},
            device_id_type=MESH,
        )

    def take_weight(which, source):
        return pltpu.make_async_remote_copy(
            src_ref=weights[which],
            dst_ref=natural.at[which, rows_of(source)],
            send_sem=cs.at[which, source],
            recv_sem=cr.at[which, source],
            device_id={"band": source},
            device_id_type=MESH,
        )

    def relay_weight(which, source, to):
        return pltpu.make_async_remote_copy(
            src_ref=natural.at[which, rows_of(source)],
            dst_ref=natural.at[which, rows_of(source)],
            send_sem=rs.at[which, source],
            recv_sem=cr.at[which, source],
            device_id={"band": to},
            device_id_type=MESH,
        )

    def own_weight(which):
        return pltpu.make_async_copy(weights[which], natural.at[which, rows_of(me)], co.at[which])

    def send_result(group, to):
        return pltpu.make_async_remote_copy(
            src_ref=fields.at[group, band_of(to)],
            dst_ref=out.at[group * ways + me],
            send_sem=bs.at[group, to],
            recv_sem=br.at[group, me],
            device_id={"band": to},
            device_id_type=MESH,
        )

    def take_result(group, source):
        return pltpu.make_async_remote_copy(
            src_ref=fields.at[group, band_of(source)],
            dst_ref=out.at[group * ways + source],
            send_sem=bs.at[group, source],
            recv_sem=br.at[group, source],
            device_id={"band": source},
            device_id_type=MESH,
        )

    def own_result(group):
        return pltpu.make_async_copy(
            fields.at[group, band_of(me)], out.at[group * ways + me], bo.at[group]
        )

    def step_partner(step):
        return partner((step // cores + 1) % chips, cores - 1 - step % cores)

    barrier = pltpu.get_barrier_semaphore()
    for step in range(ways - 1):
        pl.semaphore_signal(barrier, inc=1, device_id={"band": step_partner(step)}, device_id_type=MESH)
    pl.semaphore_wait(barrier, ways - 1)

    def start_fields(group):
        for step in range(ways - 1):
            send_field(group, step_partner(step)).start()
        own_field(group).start()

    start_fields(0)
    seeded = [
        pltpu.make_async_copy(source, target, ss.at[number])
        for number, (source, target) in enumerate(
            ((seed_cr, coarse_r), (seed_fr, fine_r), (seed_cl, coarse_l), (seed_fl, fine_l))
        )
    ]
    for copy in seeded:
        copy.start()
    for which in range(2):
        for away in range(1, chips):
            send_weight(which, partner(away, 0)).start()
        for side in range(1, cores):
            send_weight(which, partner(0, side)).start()
        own_weight(which).start()
    for group in range(1, groups):
        start_fields(group)

    for copy in seeded:
        copy.wait()

    def rows_table(block, _):
        one, at = pl.ds(block, 1), pl.ds(pl.multiple_of(block * ROWS, ROWS), ROWS)
        cos_u, sin_u = coarse_r[0, one, :], coarse_r[1, one, :]
        cos_v, sin_v = fine_r[0], fine_r[1]
        high, low = split(cos_u * cos_v - sin_u * sin_v)
        basis_h[at, :half], basis_l[at, :half] = high, low
        high, low = split(sin_u * cos_v + cos_u * sin_v)
        basis_h[at, half:], basis_l[at, half:] = high, low
        return _

    lax.fori_loop(0, cells // ROWS, rows_table, 0)
    chunk = half // 6 if half % 96 == 0 else half

    def lanes_table(block, _):
        at = pl.ds(pl.multiple_of(block * chunk, chunk), chunk)
        below = pl.ds(pl.multiple_of(half + block * chunk, chunk), chunk)
        cos_v, sin_v = fine_l[0, at, :], fine_l[1, at, :]
        cos_w, sin_w = coarse_l[0, at, :], coarse_l[1, at, :]
        for word in range(cells // LANES):
            lanes = slice(word * LANES, (word + 1) * LANES)
            cos_u, sin_u = cos_w[:, word : word + 1], sin_w[:, word : word + 1]
            high, low = split(cos_u * cos_v - sin_u * sin_v)
            basis_th[at, lanes], basis_tl[at, lanes] = high, low
            high, low = split(sin_u * cos_v + cos_u * sin_v)
            basis_th[below, lanes], basis_tl[below, lanes] = high, low
        return _

    lax.fori_loop(0, half // chunk, lanes_table, 0)

    def factor(index):
        wave = jnp.where(index < half, index, index - half)
        return jnp.where(wave == 0, 1.0, 2.0) / cells

    def tile(index):
        return pl.ds(pl.multiple_of(index * TILE, TILE), TILE)

    def one_level(group, first):
        for step in range(ways - 1):
            take_field(group, step_partner(step)).wait_recv()
        own_field(group).wait()

        def split_field(index, _):
            at = band_of(index)
            field_h[at, :], field_l[at, :] = split(fields[group, at, :])
            return _

        lax.fori_loop(0, ways, split_field, 0)

        def synth_x(index, _):
            at = tile(index)
            value = dot3(basis_h[at, :], basis_l[at, :], field_h[...], field_l[...])
            half_h[at, :], half_l[at, :] = split(value)
            return _

        lax.fori_loop(0, cells // TILE, synth_x, 0)

        if first:
            for which in range(2):
                for away in range(1, chips):
                    take_weight(which, partner(away, 0)).wait_recv()
                    for side in range(1, cores):
                        relay_weight(which, partner(away, 0), partner(0, side)).start()
                for side in range(1, cores):
                    take_weight(which, partner(0, side)).wait_recv()
                own_weight(which).wait()
            for which in range(2):
                for away in range(1, chips):
                    for side in range(1, cores):
                        take_weight(which, partner(away, side)).wait_recv()
                        relay_weight(which, partner(away, 0), partner(0, side)).wait_send()

                def turn(index, _):
                    at = pl.ds(pl.multiple_of(index * LANES, LANES), LANES)
                    value = natural[which, at, :].T
                    turned[which, :, at] = value * (1.0 / half) if which == 0 else value
                    return _

                lax.fori_loop(0, cells // LANES, turn, 0)

        total[...] = jnp.zeros_like(total)

        def synth_y(index, _):
            at = tile(index)
            value = dot3(half_h[at, :], half_l[at, :], basis_th[...], basis_tl[...])
            value = value * turned[0, at, :]
            natural[0, at, :] = value
            total[...] += jnp.sum((value * value).reshape(TILE // 8, 8, cells), axis=0)
            return _

        lax.fori_loop(0, cells // TILE, synth_y, 0)
        energy = jnp.sum(jnp.sum(total[...], axis=0, keepdims=True), axis=1, keepdims=True)
        scale = 1.0 / jnp.sqrt(energy * (1.0 / (cells * cells)) + 1e-06)

        def nonlinear(index, _):
            at = tile(index)
            scaled = natural[0, at, :] * scale
            tend_h[at, :], tend_l[at, :] = split(scaled + turned[1, at, :] * scaled * scaled)
            return _

        lax.fori_loop(0, cells // TILE, nonlinear, 0)

        def analyse_x(index, _):
            at = tile(index)
            value = dot3(basis_th[at, :], basis_tl[at, :], tend_h[...], tend_l[...])
            back_h[at, :], back_l[at, :] = split(value)
            return _

        lax.fori_loop(0, coeffs // TILE, analyse_x, 0)
        columns = factor(lax.broadcasted_iota(jnp.int32, (1, coeffs), 1)) * half

        def analyse_y(step, _):
            to = step_partner(step)
            at = band_of(to)
            value = dot3(back_h[at, :], back_l[at, :], basis_h[...], basis_l[...])
            line = factor(lax.broadcasted_iota(jnp.int32, (band, 1), 0) + to * band)
            fields[group, at, :] = value * (line * columns)

            @pl.when(step > 0)
            def _send():
                send_result(group, step_partner(step - 1)).start()

            return _

        lax.fori_loop(0, ways, analyse_y, 0)
        own_result(group).start()

    one_level(0, True)
    if groups > 1:

        def later(group, _):
            one_level(group, False)
            return _

        lax.fori_loop(1, groups, later, 0)

    def finish(group, _):
        for step in range(ways - 1):
            other = step_partner(step)
            send_field(group, other).wait_send()
            send_result(group, other).wait_send()
            take_result(group, other).wait_recv()
        own_result(group).wait()
        return _

    for which in range(2):
        for away in range(1, chips):
            send_weight(which, partner(away, 0)).wait_send()
        for side in range(1, cores):
            send_weight(which, partner(0, side)).wait_send()
    lax.fori_loop(0, groups, finish, 0)


def on_device(spectral, coupling, quadratic):
    levels, band, coeffs = spectral.shape
    rows, cells = coupling.shape
    ways = lax.axis_size("band")
    groups = levels // ways
    anywhere = pl.BlockSpec(memory_space=pltpu.HBM)
    inside = pl.BlockSpec(memory_space=pltpu.VMEM)
    tables = seeds(cells, coeffs)
    copies = pltpu.SemaphoreType.DMA
    return pl.pallas_call(
        functools.partial(round_trip, ways),
        out_shape=pltpu.VMEM((levels, band, coeffs), F32),
        in_specs=[anywhere] * 7,
        out_specs=inside,
        scratch_shapes=[
            *(pltpu.VMEM(table.shape, F32) for table in tables),
            pltpu.VMEM((groups, coeffs, coeffs), F32),
            pltpu.VMEM((2, cells, cells), F32),
            pltpu.VMEM((2, cells, cells), F32),
            pltpu.VMEM((cells, coeffs), BF16),
            pltpu.VMEM((cells, coeffs), BF16),
            pltpu.VMEM((coeffs, cells), BF16),
            pltpu.VMEM((coeffs, cells), BF16),
            pltpu.VMEM((coeffs, coeffs), BF16),
            pltpu.VMEM((coeffs, coeffs), BF16),
            pltpu.VMEM((cells, coeffs), BF16),
            pltpu.VMEM((cells, coeffs), BF16),
            pltpu.VMEM((cells, cells), BF16),
            pltpu.VMEM((cells, cells), BF16),
            pltpu.VMEM((coeffs, cells), BF16),
            pltpu.VMEM((coeffs, cells), BF16),
            pltpu.VMEM((8, cells), F32),
            copies((len(tables),)),
            copies((groups, ways)),
            copies((groups, ways)),
            copies((groups,)),
            copies((2, ways)),
            copies((2, ways)),
            copies((2,)),
            copies((2, ways)),
            copies((groups, ways)),
            copies((groups, ways)),
            copies((groups,)),
        ],
        compiler_params=pltpu.CompilerParams(
            collective_id=0, has_side_effects=True, vmem_limit_bytes=50 * 2**20
        ),
        name="round_trip",
    )(spectral, coupling, quadratic, *tables)


def solution(mesh):
    placed = (P("member", "band", None), P(("member", "band"), None), P(("member", "band"), None))
    return jax.shard_map(
        on_device, mesh=mesh, in_specs=placed, out_specs=P("member", "band", None), check_vma=False
    )
```

```python
import functools
import math

import jax
import jax.numpy as jnp
import numpy as np
from jax import lax
from jax.experimental import pallas as pl
from jax.experimental.pallas import tpu as pltpu
from jax.sharding import PartitionSpec as P

MESH = pl.DeviceIdType.MESH
F32 = jnp.float32
BF16 = jnp.bfloat16
LANES = 128
ROWS = 32
TILE = 256
PIECES = 4
SHARED = 2
EARLY = 1


def seeds(cells, coeffs):
    half = coeffs // 2
    wave = np.arange(half)

    def pair(points, transposed):
        turns = np.outer(points, wave) % cells
        angles = turns * (2.0 * math.pi / cells)
        both = np.stack([np.cos(angles), np.sin(angles)])
        return np.swapaxes(both, 1, 2).astype(np.float32) if transposed else both.astype(np.float32)

    return (
        pair(np.arange(0, cells, ROWS), False),
        pair(np.arange(ROWS), False),
        pair(np.arange(0, cells, LANES), True),
        pair(np.arange(LANES), True),
    )


def split(value):
    high = value.astype(BF16)
    return high, (value - high.astype(F32)).astype(BF16)


def dot3(a_high, a_low, b_high, b_low):
    dot = functools.partial(jnp.dot, preferred_element_type=F32)
    return dot(a_high, b_high) + dot(a_low, b_high) + dot(a_high, b_low)


def round_trip(
    ways, spectral, coupling, quadratic, seed_cr, seed_fr, seed_cl, seed_fl, out,
    coarse_r, fine_r, coarse_l, fine_l, fields, natural, turned, basis_h, basis_l, basis_th, basis_tl,
    field_h, field_l, half_h, half_l, tend_h, tend_l, back_h, back_l, total,
    ss, fs, fr, fo, cs, cr, co, rs, bs, br, bo,
):
    levels, band, coeffs = spectral.shape
    rows, cells = coupling.shape
    half = coeffs // 2
    groups = levels // ways
    cores = 2 if ways % 2 == 0 else 1
    chips = ways // cores
    me = lax.axis_index("band")
    chip, core = me // cores, me % cores

    def partner(away, side):
        return ((chip + away) % chips) * cores + (core + side) % cores

    def band_of(index):
        return pl.ds(pl.multiple_of(index * band, band), band)

    def rows_of(index):
        return pl.ds(pl.multiple_of(index * rows, rows), rows)

    def send_field(group, to):
        return pltpu.make_async_remote_copy(
            src_ref=spectral.at[group * ways + to],
            dst_ref=fields.at[group, band_of(me)],
            send_sem=fs.at[group, to],
            recv_sem=fr.at[group, me],
            device_id={"band": to},
            device_id_type=MESH,
        )

    def take_field(group, source):
        return pltpu.make_async_remote_copy(
            src_ref=spectral.at[group * ways + me],
            dst_ref=fields.at[group, band_of(source)],
            send_sem=fs.at[group, source],
            recv_sem=fr.at[group, source],
            device_id={"band": source},
            device_id_type=MESH,
        )

    def own_field(group):
        return pltpu.make_async_copy(
            spectral.at[group * ways + me], fields.at[group, band_of(me)], fo.at[group]
        )

    weights = (coupling, quadratic)

    def send_weight(which, to):
        return pltpu.make_async_remote_copy(
            src_ref=weights[which],
            dst_ref=natural.at[which, rows_of(me)],
            send_sem=cs.at[which, to],
            recv_sem=cr.at[which, me],
            device_id={"band": to},
            device_id_type=MESH,
        )

    def take_weight(which, source):
        return pltpu.make_async_remote_copy(
            src_ref=weights[which],
            dst_ref=natural.at[which, rows_of(source)],
            send_sem=cs.at[which, source],
            recv_sem=cr.at[which, source],
            device_id={"band": source},
            device_id_type=MESH,
        )

    def relay_weight(which, source, to):
        return pltpu.make_async_remote_copy(
            src_ref=natural.at[which, rows_of(source)],
            dst_ref=natural.at[which, rows_of(source)],
            send_sem=rs.at[which, source],
            recv_sem=cr.at[which, source],
            device_id={"band": to},
            device_id_type=MESH,
        )

    def own_weight(which):
        return pltpu.make_async_copy(weights[which], natural.at[which, rows_of(me)], co.at[which])

    def send_result(group, to):
        return pltpu.make_async_remote_copy(
            src_ref=fields.at[group, band_of(to)],
            dst_ref=out.at[group * ways + me],
            send_sem=bs.at[group, to],
            recv_sem=br.at[group, me],
            device_id={"band": to},
            device_id_type=MESH,
        )

    def take_result(group, source):
        return pltpu.make_async_remote_copy(
            src_ref=fields.at[group, band_of(source)],
            dst_ref=out.at[group * ways + source],
            send_sem=bs.at[group, source],
            recv_sem=br.at[group, source],
            device_id={"band": source},
            device_id_type=MESH,
        )

    def own_result(group):
        return pltpu.make_async_copy(
            fields.at[group, band_of(me)], out.at[group * ways + me], bo.at[group]
        )

    def step_partner(step):
        return partner((step // cores + 1) % chips, cores - 1 - step % cores)

    barrier = pltpu.get_barrier_semaphore()
    for step in range(ways - 1):
        pl.semaphore_signal(barrier, inc=1, device_id={"band": step_partner(step)}, device_id_type=MESH)
    pl.semaphore_wait(barrier, ways - 1)

    def start_fields(group):
        for step in range(ways - 1):
            send_field(group, step_partner(step)).start()
        own_field(group).start()

    start_fields(0)
    seeded = [
        pltpu.make_async_copy(source, target, ss.at[number])
        for number, (source, target) in enumerate(
            ((seed_cr, coarse_r), (seed_fr, fine_r), (seed_cl, coarse_l), (seed_fl, fine_l))
        )
    ]
    for copy in seeded:
        copy.start()
    for which in range(2):
        for away in range(1, chips):
            send_weight(which, partner(away, 0)).start()
        for side in range(1, cores):
            send_weight(which, partner(0, side)).start()
        own_weight(which).start()
    for group in range(1, groups):
        start_fields(group)

    for copy in seeded:
        copy.wait()

    def rows_table(block, _):
        one, at = pl.ds(block, 1), pl.ds(pl.multiple_of(block * ROWS, ROWS), ROWS)
        cos_u, sin_u = coarse_r[0, one, :], coarse_r[1, one, :]
        cos_v, sin_v = fine_r[0], fine_r[1]
        high, low = split(cos_u * cos_v - sin_u * sin_v)
        basis_h[at, :half], basis_l[at, :half] = high, low
        high, low = split(sin_u * cos_v + cos_u * sin_v)
        basis_h[at, half:], basis_l[at, half:] = high, low
        return _

    lax.fori_loop(0, cells // ROWS, rows_table, 0)
    chunk = half // 6 if half % 96 == 0 else half

    def lanes_table(block, _):
        at = pl.ds(pl.multiple_of(block * chunk, chunk), chunk)
        below = pl.ds(pl.multiple_of(half + block * chunk, chunk), chunk)
        cos_v, sin_v = fine_l[0, at, :], fine_l[1, at, :]
        cos_w, sin_w = coarse_l[0, at, :], coarse_l[1, at, :]
        for word in range(cells // LANES):
            lanes = slice(word * LANES, (word + 1) * LANES)
            cos_u, sin_u = cos_w[:, word : word + 1], sin_w[:, word : word + 1]
            high, low = split(cos_u * cos_v - sin_u * sin_v)
            basis_th[at, lanes], basis_tl[at, lanes] = high, low
            high, low = split(sin_u * cos_v + cos_u * sin_v)
            basis_th[below, lanes], basis_tl[below, lanes] = high, low
        return _

    lax.fori_loop(0, half // chunk, lanes_table, 0)

    def factor(index):
        wave = jnp.where(index < half, index, index - half)
        return jnp.where(wave == 0, 1.0, 2.0) / cells

    def tile(index):
        return pl.ds(pl.multiple_of(index * TILE, TILE), TILE)

    def one_level(group, first):
        for step in range(ways - 1):
            take_field(group, step_partner(step)).wait_recv()
        own_field(group).wait()

        def split_field(index, _):
            at = band_of(index)
            field_h[at, :], field_l[at, :] = split(fields[group, at, :])
            return _

        lax.fori_loop(0, ways, split_field, 0)

        def synth_x(index, _):
            at = tile(index)
            value = dot3(basis_h[at, :], basis_l[at, :], field_h[...], field_l[...])
            half_h[at, :], half_l[at, :] = split(value)
            return _

        lax.fori_loop(0, cells // TILE, synth_x, 0)

        if first:
            for which in range(2):
                for away in range(1, chips):
                    take_weight(which, partner(away, 0)).wait_recv()
                    for side in range(1, cores):
                        relay_weight(which, partner(away, 0), partner(0, side)).start()
                for side in range(1, cores):
                    take_weight(which, partner(0, side)).wait_recv()
                own_weight(which).wait()
            for which in range(2):
                for away in range(1, chips):
                    for side in range(1, cores):
                        take_weight(which, partner(away, side)).wait_recv()
                        relay_weight(which, partner(away, 0), partner(0, side)).wait_send()

                def turn(index, _):
                    at = pl.ds(pl.multiple_of(index * LANES, LANES), LANES)
                    value = natural[which, at, :].T
                    turned[which, :, at] = value * (1.0 / half) if which == 0 else value
                    return _

                lax.fori_loop(0, cells // LANES, turn, 0)

        total[...] = jnp.zeros_like(total)

        def synth_y(index, _):
            at = tile(index)
            value = dot3(half_h[at, :], half_l[at, :], basis_th[...], basis_tl[...])
            value = value * turned[0, at, :]
            natural[0, at, :] = value
            total[...] += jnp.sum((value * value).reshape(TILE // 8, 8, cells), axis=0)
            return _

        lax.fori_loop(0, cells // TILE, synth_y, 0)
        energy = jnp.sum(jnp.sum(total[...], axis=0, keepdims=True), axis=1, keepdims=True)
        scale = 1.0 / jnp.sqrt(energy * (1.0 / (cells * cells)) + 1e-06)

        def nonlinear(index, _):
            at = tile(index)
            scaled = natural[0, at, :] * scale
            tend_h[at, :], tend_l[at, :] = split(scaled + turned[1, at, :] * scaled * scaled)
            return _

        lax.fori_loop(0, cells // TILE, nonlinear, 0)

        def analyse_x(index, _):
            at = tile(index)
            value = dot3(basis_th[at, :], basis_tl[at, :], tend_h[...], tend_l[...])
            back_h[at, :], back_l[at, :] = split(value)
            return _

        lax.fori_loop(0, coeffs // TILE, analyse_x, 0)
        columns = factor(lax.broadcasted_iota(jnp.int32, (1, coeffs), 1)) * half

        def analyse_y(step, _):
            to = step_partner(step)
            at = band_of(to)
            value = dot3(back_h[at, :], back_l[at, :], basis_h[...], basis_l[...])
            line = factor(lax.broadcasted_iota(jnp.int32, (band, 1), 0) + to * band)
            fields[group, at, :] = value * (line * columns)

            @pl.when(step > 0)
            def _send():
                send_result(group, step_partner(step - 1)).start()

            return _

        lax.fori_loop(0, ways, analyse_y, 0)
        own_result(group).start()

    one_level(0, True)
    if groups > 1:

        def later(group, _):
            one_level(group, False)
            return _

        lax.fori_loop(1, groups, later, 0)

    def finish(group, _):
        for step in range(ways - 1):
            other = step_partner(step)
            send_field(group, other).wait_send()
            send_result(group, other).wait_send()
            take_result(group, other).wait_recv()
        own_result(group).wait()
        return _

    for which in range(2):
        for away in range(1, chips):
            send_weight(which, partner(away, 0)).wait_send()
        for side in range(1, cores):
            send_weight(which, partner(0, side)).wait_send()
    lax.fori_loop(0, groups, finish, 0)


def on_device(spectral, coupling, quadratic):
    levels, band, coeffs = spectral.shape
    rows, cells = coupling.shape
    ways = lax.axis_size("band")
    groups = levels // ways
    anywhere = pl.BlockSpec(memory_space=pltpu.HBM)
    inside = pl.BlockSpec(memory_space=pltpu.VMEM)
    tables = seeds(cells, coeffs)
    copies = pltpu.SemaphoreType.DMA
    return pl.pallas_call(
        functools.partial(round_trip, ways),
        out_shape=pltpu.VMEM((levels, band, coeffs), F32),
        in_specs=[anywhere] * 7,
        out_specs=inside,
        scratch_shapes=[
            *(pltpu.VMEM(table.shape, F32) for table in tables),
            pltpu.VMEM((groups, coeffs, coeffs), F32),
            pltpu.VMEM((2, cells, cells), F32),
            pltpu.VMEM((2, cells, cells), F32),
            pltpu.VMEM((cells, coeffs), BF16),
            pltpu.VMEM((cells, coeffs), BF16),
            pltpu.VMEM((coeffs, cells), BF16),
            pltpu.VMEM((coeffs, cells), BF16),
            pltpu.VMEM((coeffs, coeffs), BF16),
            pltpu.VMEM((coeffs, coeffs), BF16),
            pltpu.VMEM((cells, coeffs), BF16),
            pltpu.VMEM((cells, coeffs), BF16),
            pltpu.VMEM((cells, cells), BF16),
            pltpu.VMEM((cells, cells), BF16),
            pltpu.VMEM((coeffs, cells), BF16),
            pltpu.VMEM((coeffs, cells), BF16),
            pltpu.VMEM((8, cells), F32),
            copies((len(tables),)),
            copies((groups, ways)),
            copies((groups, ways)),
            copies((groups,)),
            copies((2, ways)),
            copies((2, ways)),
            copies((2,)),
            copies((2, ways)),
            copies((groups, ways)),
            copies((groups, ways)),
            copies((groups,)),
        ],
        compiler_params=pltpu.CompilerParams(
            collective_id=0, has_side_effects=True, vmem_limit_bytes=50 * 2**20
        ),
        name="round_trip",
    )(spectral, coupling, quadratic, *tables)


def paired(
    spectral, coupling, quadratic, seed_cr, seed_fr, seed_cl, seed_fl, out, natural,
    coarse_r, fine_r, coarse_l, fine_l, fields, landed, turned, basis_h, basis_l, basis_th, basis_tl,
    wide_h, wide_l, side_h, side_l, product, staged, total,
    ss, fs, fr, fo, gs, ls, lr, ws, kr, cs, cr, co, rs, xs, bs, br, bo,
):
    levels, band, coeffs = spectral.shape
    rows, cells = coupling.shape
    half = coeffs // 2
    home, guest = levels * 3 // 8, levels // 8
    piece = band // PIECES
    guests = 2 * guest * PIECES
    tail = pl.ds(SHARED * piece, band - SHARED * piece)
    member, me = lax.axis_index("member"), lax.axis_index("band")
    m, x, c = member % 2, me // 2, me % 2
    near = m == x
    far = m != x
    same = 1 - (m - x) * (m - x)
    weights = (coupling, quadratic)

    def device(row, column, core):
        return {"member": member - m + row, "band": column * 2 + core}

    def remote(source, target, sent, received, to):
        return pltpu.make_async_remote_copy(
            src_ref=source, dst_ref=target, send_sem=sent, recv_sem=received,
            device_id=to, device_id_type=MESH,
        )

    def band_of(index):
        return pl.ds(pl.multiple_of(index * band, band), band)

    def part_of(index, number):
        return pl.ds(pl.multiple_of(index * band + number * piece, piece), piece)

    def tail_of(index):
        return pl.ds(pl.multiple_of(index * band + SHARED * piece, piece), band - SHARED * piece)

    def rows_of(index):
        return pl.ds(pl.multiple_of(index * rows, rows), rows)

    sibling = device(m, x, 1 - c)
    def near_sibling(slot):
        return remote(
            spectral.at[(1 - c) * home + slot], fields.at[slot, band_of(me)],
            fs.at[slot, 0], fr.at[slot, me], sibling,
        )

    def near_own(slot):
        return pltpu.make_async_copy(
            spectral.at[c * home + slot], fields.at[slot, band_of(me)], fo.at[slot]
        )

    def near_guest(slot, core):
        return remote(
            spectral.at[2 * home + core * guest + slot], fields.at[slot, band_of(me)],
            gs.at[slot, core], fr.at[slot, me], device(1 - m, x, core),
        )

    def far_home(slot, core):
        return remote(
            spectral.at[core * home + slot], fields.at[slot, band_of(me)],
            fs.at[slot, core], fr.at[slot, me], device(m, 1 - x, core),
        )

    def far_tail(core):
        slot = EARLY
        return remote(
            spectral.at[core * home + slot, tail], fields.at[slot, tail_of(me)],
            fs.at[slot, core], fr.at[slot, me], device(m, 1 - x, core),
        )

    def far_piece(number):
        if number < guests:
            slot, core, part = number // (2 * PIECES), number // PIECES % 2, number % PIECES
            level = 2 * home + core * guest + slot
        else:
            core, part = (number - guests) // SHARED, (number - guests) % SHARED
            level = core * home + EARLY
        return remote(
            spectral.at[level, pl.ds(part * piece, piece)], landed.at[number],
            ls.at[number], lr.at[number], device(1 - m, x, c),
        )

    def forward(number, target, to):
        @pl.when(near)
        def _forward():
            far_piece_landed(number).wait_recv()
            remote(landed.at[number], target, ws.at[number], kr.at[number, c], to).start()

    def far_piece_landed(number):
        return remote(
            landed.at[number], landed.at[number], ls.at[number], lr.at[number], device(1 - m, x, c)
        )

    def forwarded(number):
        return remote(
            landed.at[number], landed.at[number], ws.at[number], kr.at[number, c], sibling
        )

    def forward_guest(number):
        slot, core, part = number // (2 * PIECES), number // PIECES % 2, number % PIECES
        forward(number, fields.at[slot, part_of(me, part)], device(m, 1 - x, core))

    def forward_home(index):
        core, part = index // SHARED, index % SHARED
        forward(
            guests + index, fields.at[EARLY, part_of(me, part)], device(1 - m, 1 - x, core)
        )

    def taken(target, received):
        return remote(target, target, ss.at[0], received, sibling)

    def take_fields(slot):
        @pl.when(near)
        def _home():
            near_own(slot).wait()
            other = 2 * x + 1 - c
            taken(fields.at[slot, band_of(other)], fr.at[slot, other]).wait_recv()

            @pl.when(slot != EARLY)
            def _whole():
                for core in range(2):
                    source = 2 * (1 - x) + core
                    taken(fields.at[slot, band_of(source)], fr.at[slot, source]).wait_recv()

            @pl.when(slot == EARLY)
            def _parts():
                for core in range(2):
                    source = 2 * (1 - x) + core
                    taken(fields.at[slot, tail_of(source)], fr.at[slot, source]).wait_recv()
                    for part in range(SHARED):
                        number = guests + c * SHARED + part
                        taken(fields.at[slot, part_of(source, part)], kr.at[number, core]).wait_recv()

        @pl.when(far)
        def _guest():
            for core in range(2):
                source = 2 * x + core
                taken(fields.at[slot, band_of(source)], fr.at[slot, source]).wait_recv()
                source = 2 * (1 - x) + core
                for part in range(PIECES):
                    number = (slot * 2 + c) * PIECES + part
                    taken(fields.at[slot, part_of(source, part)], kr.at[number, core]).wait_recv()

    def give(which, number, to):
        return remote(
            weights[which], natural.at[which, rows_of(me)], cs.at[which, number], cr.at[which, me], to
        )

    def weight(which, source):
        at = natural.at[which, rows_of(source)]
        return taken(at, cr.at[which, source])

    def relay(which, source, number, to):
        at = natural.at[which, rows_of(source)]
        return remote(at, at, rs.at[which, number], cr.at[which, source], to)

    close, remote_band = 2 * x + c, 2 * (1 - x) + c

    def stage(which, column):
        copy = pltpu.make_async_copy(
            natural.at[which, pl.ds(pl.multiple_of(column * 2 * rows, 2 * rows), 2 * rows)],
            staged, xs.at[which, column],
        )
        copy.start()
        copy.wait()

    def gather_close(which):
        other = 2 * x + 1 - c

        @pl.when(near)
        def _home():
            own = pltpu.make_async_copy(weights[which], staged.at[rows_of(c)], co.at[which])
            own.start()
            weight(which, other).wait_recv()
            rest = pltpu.make_async_copy(
                natural.at[which, rows_of(other)], staged.at[rows_of(1 - c)], xs.at[which, 0]
            )
            rest.start()
            own.wait()
            rest.wait()

        @pl.when(far)
        def _guest():
            weight(which, close).wait_recv()
            relay(which, close, 0, sibling).start()
            weight(which, other).wait_recv()
            stage(which, x)

    def gather_remote(which):
        weight(which, remote_band).wait_recv()
        relay(which, remote_band, 1, sibling).start()

        @pl.when(near)
        def _home():
            relay(which, remote_band, 0, device(1 - m, x, c)).start()

        weight(which, 2 * (1 - x) + 1 - c).wait_recv()
        stage(which, 1 - x)

    def level_of(slot):
        return same * (c * home + slot) + (1 - same) * (2 * home + c * guest + slot)

    def target_of(step):
        column = (1 - x) + (step // 2) * (2 * x - 1)
        core = step // 2 * (1 - c) + step % 2 * (1 + step // 2 * (2 * c - 2))
        return column, core

    def give_result(slot, step):
        column, core = target_of(step)
        return remote(
            fields.at[slot, band_of(column * 2 + core)], out.at[level_of(slot)],
            bs.at[slot, step], br.at[level_of(slot)], device(x, column, core),
        )

    def own_result(slot):
        return pltpu.make_async_copy(
            fields.at[slot, band_of(me)], out.at[c * home + slot], bo.at[slot]
        )

    def result(level):
        return taken(out.at[level], br.at[level])

    barrier = pltpu.get_barrier_semaphore()
    others = [device(m, x, 1 - c)]
    others += [device(row, column, core) for row, column in ((m, 1 - x), (1 - m, x), (1 - m, 1 - x)) for core in range(2)]
    for other in others:
        pl.semaphore_signal(barrier, inc=1, device_id=other, device_id_type=MESH)
    pl.semaphore_wait(barrier, len(others))

    @pl.when(far)
    def _start_far():
        across = [(band * coeffs, far_home(0, core)) for core in (c, 1 - c)]
        across += [(rows * cells, give(which, 0, device(m, 1 - x, c))) for which in range(2)]
        across += [((band - SHARED * piece) * coeffs, far_tail(core)) for core in (c, 1 - c)]
        for slot in range(home):
            if slot not in (0, EARLY):
                across += [(band * coeffs, far_home(slot, core)) for core in (c, 1 - c)]
        along = [(piece * coeffs, far_piece(number)) for number in range(guests + 2 * SHARED)]
        order = []
        for line, entries in enumerate((along, across)):
            begin = 0
            for size, copy in entries:
                order.append((begin, line, copy))
                begin += size
        for _, _, copy in sorted(order, key=lambda entry: entry[:2]):
            copy.start()

    @pl.when(near)
    def _start_near():
        for which in range(2):
            give(which, 1, device(1 - m, x, c)).start()
            give(which, 0, sibling).start()
        for slot in range(home):
            near_sibling(slot).start()
            near_own(slot).start()

    seeded = [
        pltpu.make_async_copy(source, target, ss.at[1 + number])
        for number, (source, target) in enumerate(
            ((seed_cr, coarse_r), (seed_fr, fine_r), (seed_cl, coarse_l), (seed_fl, fine_l))
        )
    ]
    for copy in seeded:
        copy.start()
    for copy in seeded:
        copy.wait()

    def rows_table(block):
        one, at = pl.ds(block, 1), pl.ds(pl.multiple_of(block * ROWS, ROWS), ROWS)
        cos_u, sin_u = coarse_r[0, one, :], coarse_r[1, one, :]
        cos_v, sin_v = fine_r[0], fine_r[1]
        high, low = split(cos_u * cos_v - sin_u * sin_v)
        basis_h[at, :half], basis_l[at, :half] = high, low
        high, low = split(sin_u * cos_v + cos_u * sin_v)
        basis_h[at, half:], basis_l[at, half:] = high, low

    chunk = half // 8

    def lanes_table(block):
        at = pl.ds(pl.multiple_of(block * chunk, chunk), chunk)
        below = pl.ds(pl.multiple_of(half + block * chunk, chunk), chunk)
        cos_v, sin_v = fine_l[0, at, :], fine_l[1, at, :]
        cos_w, sin_w = coarse_l[0, at, :], coarse_l[1, at, :]
        for word in range(cells // LANES):
            lanes = slice(word * LANES, (word + 1) * LANES)
            cos_u, sin_u = cos_w[:, word : word + 1], sin_w[:, word : word + 1]
            high, low = split(cos_u * cos_v - sin_u * sin_v)
            basis_th[at, lanes], basis_tl[at, lanes] = high, low
            high, low = split(sin_u * cos_v + cos_u * sin_v)
            basis_th[below, lanes], basis_tl[below, lanes] = high, low

    blocks = cells // ROWS // 8

    def build(index, _):
        @pl.when(index < guests // 2 - 1)
        def _send():
            forward_guest(index)

        def row(number, _):
            rows_table(index * blocks + number)
            return _

        lax.fori_loop(0, blocks, row, 0)
        lanes_table(index)
        return _

    lax.fori_loop(0, 8, build, 0)
    def forward_next(number, last):
        @pl.when((number < guests) & (number < last))
        def _send():
            forward_guest(number)

        @pl.when((number >= guests) & (number < last))
        def _send_home():
            forward_home(number - guests)

    def turn(which, column, factor, number, last):
        def one(index, _):
            forward_next(number + index, last)
            at = pl.ds(pl.multiple_of(index * LANES, LANES), LANES)
            to = pl.ds(pl.multiple_of(column * 2 * rows + index * LANES, LANES), LANES)
            value = staged[at, :].T
            turned[which, :, to] = value * factor if which == 0 else value
            return _

        lax.fori_loop(0, 2 * rows // LANES, one, 0)

    pieces = guests + 2 * SHARED
    gather_close(0)
    turn(0, x, 1.0 / half, 7, 9)
    gather_close(1)
    turn(1, x, 1.0, 9, 11)

    def factor(index):
        wave = jnp.where(index < half, index, index - half)
        return jnp.where(wave == 0, 1.0, 2.0) / cells

    def tile(index):
        return pl.ds(pl.multiple_of(index * TILE, TILE), TILE)

    def one_level(slot, first):
        take_fields(slot)

        def split_field(index, _):
            at = band_of(index)
            wide_h[at, :coeffs], wide_l[at, :coeffs] = split(fields[slot, at, :])
            return _

        lax.fori_loop(0, coeffs // band, split_field, 0)

        def synth_x(index, _):
            if first:
                forward_next(11 + index, 14)
            at = tile(index)
            value = dot3(
                basis_h[at, :], basis_l[at, :], wide_h[:coeffs, :coeffs], wide_l[:coeffs, :coeffs]
            )
            side_h[at, :coeffs], side_l[at, :coeffs] = split(value)
            return _

        steps = cells // TILE
        lax.fori_loop(0, steps, synth_x, 0)
        if first:
            gather_remote(0)
            turn(0, 1 - x, 1.0 / half, 14, 16)
        total[...] = jnp.zeros_like(total)

        def synth_y(index, _):
            if first:
                @pl.when(index >= steps // 2)
                def _send():
                    forward_next(16 - steps // 2 + index, 18)

            at = tile(index)
            value = dot3(side_h[at, :coeffs], side_l[at, :coeffs], basis_th[...], basis_tl[...])
            value = value * turned[0, at, :]
            product[at, :] = value
            total[...] += jnp.sum((value * value).reshape(TILE // 8, 8, cells), axis=0)
            return _

        lax.fori_loop(0, steps, synth_y, 0)
        if first:
            gather_remote(1)

            @pl.when(near)
            def _start_guest():
                for other in range(guest):
                    for core in range(2):
                        near_guest(other, core).start()

            turn(1, 1 - x, 1.0, 0, 0)
        energy = jnp.sum(jnp.sum(total[...], axis=0, keepdims=True), axis=1, keepdims=True)
        scale = 1.0 / jnp.sqrt(energy * (1.0 / (cells * cells)) + 1e-06)

        def nonlinear(index, _):
            if first:
                forward_next(18 + index, pieces)
            at = tile(index)
            scaled = product[at, :] * scale
            wide_h[at, :], wide_l[at, :] = split(scaled + turned[1, at, :] * scaled * scaled)
            return _

        lax.fori_loop(0, steps, nonlinear, 0)

        columns = factor(lax.broadcasted_iota(jnp.int32, (1, coeffs), 1)) * half

        def analyse(side, _):
            column, _unused = target_of(2 * side)
            at = pl.ds(pl.multiple_of(column * half, half), half)
            value = dot3(basis_th[at, :], basis_tl[at, :], wide_h[...], wide_l[...])
            side_h[at, :], side_l[at, :] = split(value)

            def analyse_y(step, _):
                column, core = target_of(step)
                index = column * 2 + core
                at = band_of(index)
                value = dot3(side_h[at, :], side_l[at, :], basis_h[...], basis_l[...])
                line = factor(lax.broadcasted_iota(jnp.int32, (band, 1), 0) + index * band)
                fields[slot, at, :] = value * (line * columns)

                @pl.when(step > 0)
                def _send():
                    give_result(slot, step - 1).start()

                return _

            lax.fori_loop(2 * side, 2 * side + 2, analyse_y, 0)

            return _

        lax.fori_loop(0, 2, analyse, 0)

        @pl.when(near)
        def _keep():
            own_result(slot).start()

        @pl.when(far)
        def _last():
            give_result(slot, 3).start()

    one_level(0, True)

    def later(slot, _):
        one_level(slot, False)
        return _

    lax.fori_loop(1, guest + same * (home - guest), later, 0)

    @pl.when(near)
    def _finish_near():
        for which in range(2):
            give(which, 1, sibling).wait_send()
            give(which, 0, sibling).wait_send()
            relay(which, remote_band, 0, sibling).wait_send()
            relay(which, remote_band, 1, sibling).wait_send()
        for slot in range(guest):
            for core in range(2):
                near_guest(slot, core).wait_send()

        def sent(number, _):
            forwarded(number).wait_send()
            return _

        lax.fori_loop(0, guests + 2 * SHARED, sent, 0)

        def done(slot, _):
            near_sibling(slot).wait_send()
            for step in range(3):
                give_result(slot, step).wait_send()
            own_result(slot).wait()
            result((1 - c) * home + slot).wait_recv()
            return _

        lax.fori_loop(0, home, done, 0)
        for number in range(2 * guest):
            result(2 * home + number).wait_recv()

    @pl.when(far)
    def _finish_far():
        for which in range(2):
            give(which, 0, sibling).wait_send()
            relay(which, close, 0, sibling).wait_send()
            relay(which, remote_band, 1, sibling).wait_send()

        def sent(number, _):
            far_piece_landed(number).wait_send()
            return _

        lax.fori_loop(0, guests + 2 * SHARED, sent, 0)
        for slot in range(home):
            for core in range(2):
                if slot != EARLY:
                    far_home(slot, core).wait_send()
        for core in range(2):
            far_tail(core).wait_send()
        for slot in range(guest):
            for step in range(4):
                give_result(slot, step).wait_send()

        def done(level, _):
            result(level).wait_recv()
            return _

        lax.fori_loop(0, levels, done, 0)


def on_pairs(spectral, coupling, quadratic):
    levels, band, coeffs = spectral.shape
    rows, cells = coupling.shape
    home, guest = levels * 3 // 8, levels // 8
    pieces = 2 * guest * PIECES + 2 * SHARED
    away = pl.BlockSpec(memory_space=pltpu.HBM)
    inside = pl.BlockSpec(memory_space=pltpu.VMEM)
    tables = seeds(cells, coeffs)
    copies = pltpu.SemaphoreType.DMA
    return pl.pallas_call(
        paired,
        out_shape=(
            pltpu.VMEM((levels, band, coeffs), F32),
            pltpu.HBM((2, cells, cells), F32),
        ),
        in_specs=[away] * 7,
        out_specs=(inside, away),
        scratch_shapes=[
            *(pltpu.VMEM(table.shape, F32) for table in tables),
            pltpu.VMEM((home, coeffs, coeffs), F32),
            pltpu.VMEM((pieces, band // PIECES, coeffs), F32),
            pltpu.VMEM((2, cells, cells), F32),
            pltpu.VMEM((cells, coeffs), BF16),
            pltpu.VMEM((cells, coeffs), BF16),
            pltpu.VMEM((coeffs, cells), BF16),
            pltpu.VMEM((coeffs, cells), BF16),
            pltpu.VMEM((cells, cells), BF16),
            pltpu.VMEM((cells, cells), BF16),
            pltpu.VMEM((cells, cells), BF16),
            pltpu.VMEM((cells, cells), BF16),
            pltpu.VMEM((cells, cells), F32),
            pltpu.VMEM((2 * rows, cells), F32),
            pltpu.VMEM((8, cells), F32),
            copies((1 + len(tables),)),
            copies((home, 2)),
            copies((home, 4)),
            copies((home,)),
            copies((guest, 2)),
            copies((pieces,)),
            copies((pieces,)),
            copies((pieces,)),
            copies((pieces, 2)),
            copies((2, 2)),
            copies((2, 4)),
            copies((2,)),
            copies((2, 2)),
            copies((2, 2)),
            copies((home, 4)),
            copies((levels,)),
            copies((home,)),
        ],
        compiler_params=pltpu.CompilerParams(
            collective_id=1, has_side_effects=True, vmem_limit_bytes=53 * 2**20
        ),
        name="paired",
    )(spectral, coupling, quadratic, *tables)[0]


def solution(mesh):
    placed = (P("member", "band", None), P(("member", "band"), None), P(("member", "band"), None))
    pairs = mesh.shape["band"] == 4 and mesh.shape["member"] % 2 == 0
    return jax.shard_map(
        on_pairs if pairs else on_device,
        mesh=mesh,
        in_specs=placed,
        out_specs=P("member", "band", None),
        check_vma=False,
    )
```
